32 devices in a mesh: dp: 4 (over y, x), cp: 2 (over core), sp: 4 (over z).
Axes of the slice: x: 2, y: 2, z: 4, core: 2. Of those that a mesh axis runs over, the one named last changes fastest.
Arguments:
- hidden: bfloat16 [4, 4096, 1536], P('dp', ('cp', 'sp')), may hold values from -6 to 6
- norm_gain: bfloat16 [1536], P('dp'), may hold values from 0.5 to 1.5
- w_in: bfloat16 [1536, 6448], P('dp'), may hold values from -0.15625 to 0.15625
- conv_w: bfloat16 [3328, 4], P('dp'), may hold values from -3 to 3
- conv_bias: bfloat16 [3328], P('dp'), may hold values from -3 to 3
- dt_bias: float32 [48], replicated, may hold values from -6 to -1
- a_log: float32 [48], replicated, may hold values from -1 to 2.5
- d_skip: float32 [48], replicated, may hold values from 0.5 to 1.5
- gate_gain: bfloat16 [3072], P('dp'), may hold values from 0.5 to 1.5
- w_out: bfloat16 [3072, 1536], P('dp'), may hold values from -0.109375 to 0.109375
- cotangent: bfloat16 [4, 4096, 1536], P('dp', ('cp', 'sp')), may hold values from -6 to 6
Outputs:
- out_hidden: bfloat16 [4, 4096, 1536], P('dp', ('cp', 'sp'))
- grad_hidden: bfloat16 [4, 4096, 1536], P('dp', ('cp', 'sp'))
- grad_norm_gain: float32 [1536], P('dp')
- grad_w_in: float32 [1536, 6448], P('dp')
- grad_conv_w: float32 [3328, 4], P('dp')
- grad_conv_bias: float32 [3328], P('dp')
- grad_dt_bias: float32 [48], replicated
- grad_a_log: float32 [48], replicated
- grad_d_skip: float32 [48], replicated
- grad_gate_gain: float32 [3072], P('dp')
- grad_w_out: float32 [3072, 1536], P('dp')
The draws below stay inside these ranges and needn't reach their ends.
All inputs are finite; a program needn't handle non-finite values.
Results may differ from the reference program's by a relative error of at most 0.018.
Values may be sent and summed in bfloat16 or wider, within the bound.
A program may use at most 320 MiB of HBM per device.

```python
import jax
import jax.numpy as jnp
from jax import lax

D = 1536
H = 48
P_SIZE = 64
N = 128
BLOCK = 256
KW = 4
SEQ_LEN = 4096
SEQS = 4
DI = 3072
XBC = 3328
PROJ = 6448


def steps_of(key, extent, shards, smallest, high):
    gain = 1.0
    for dim, shards_of in shards:
        heights = jax.random.uniform(jax.random.fold_in(jax.random.fold_in(key, 6), dim), (shards_of,), jnp.float32, smallest / len(shards), high / len(shards))
        gain = gain * jnp.repeat(jnp.exp(heights), extent[dim] // shards_of).reshape((-1,) + (1,) * (len(extent) - 1 - dim))
    return gain


def bell_draw(stream_key, extent, width, bound, shards=(), kind=jnp.bfloat16):
    gain = steps_of(stream_key, extent, shards, -0.22, 0.18) if shards else 1.0
    values = jax.random.normal(stream_key, extent, jnp.float32) * width * gain
    return jnp.minimum(jnp.maximum(values, -bound), bound).astype(kind)


def setup_inputs(seed: int = 0) -> dict:
    streams_of = jax.random.split(jax.random.key(seed), 12)
    return {
        "hidden": bell_draw(streams_of[0], (SEQS, SEQ_LEN, D), 1.0, 6.0, ((0, 4), (1, 8))),
        "norm_gain": jnp.clip(1.0 + 0.1 * jax.random.normal(streams_of[1], (D,), jnp.float32), 0.5, 1.5).astype(jnp.bfloat16),
        "w_in": bell_draw(streams_of[2], (D, PROJ), D ** -0.5, 0.15625, ((0, 4),)),
        "conv_w": bell_draw(streams_of[3], (XBC, KW), KW ** -0.5, 3.0, ((0, 4),)),
        "conv_bias": bell_draw(streams_of[4], (XBC,), 0.5, 3.0, ((0, 4),)),
        "dt_bias": jnp.clip(jax.random.uniform(streams_of[5], (H,), jnp.float32, -6.0, -1.0), -6.0, -1.0),
        "a_log": jnp.clip(jax.random.uniform(streams_of[6], (H,), jnp.float32, -1.0, 2.5), -1.0, 2.5),
        "d_skip": jnp.clip(jax.random.uniform(streams_of[7], (H,), jnp.float32, 0.5, 1.5), 0.5, 1.5),
        "gate_gain": jnp.clip(1.0 + 0.1 * jax.random.normal(streams_of[8], (DI,), jnp.float32), 0.5, 1.5).astype(jnp.bfloat16),
        "w_out": bell_draw(streams_of[9], (DI, D), DI ** -0.5, 0.109375, ((0, 4),)),
        "cotangent": bell_draw(streams_of[10], (SEQS, SEQ_LEN, D), 1.0, 6.0, ((0, 4), (1, 8))),
    }


epsilon = 1e-05
highest = lax.Precision.HIGHEST

def state_space(values, steps, rates, inputs_b, inputs_c, skips, initial):
    batch = values.shape[0]
    length = values.shape[1]
    heads_here = values.shape[2]
    blocks = length // BLOCK
    val_blk = values.reshape(batch, blocks, BLOCK, heads_here, P_SIZE)
    step_blk = steps.reshape(batch, blocks, BLOCK, heads_here)
    cum_log = jnp.cumsum((steps * rates).reshape(batch, blocks, BLOCK, heads_here), axis=2)
    in_b = inputs_b.reshape(batch, blocks, BLOCK, N)
    in_c = inputs_c.reshape(batch, blocks, BLOCK, N)
    scores = jnp.einsum('sckn,scmn->sckm', in_c, in_b, precision=highest)
    causal = jnp.arange(BLOCK)[:, None] >= jnp.arange(BLOCK)[None, :]
    gaps = cum_log[:, :, :, None, :] - cum_log[:, :, None, :, :]
    fading = jnp.exp(jnp.where(causal[None, None, :, :, None], gaps, -jnp.inf))
    mixing = scores[..., None] * fading * step_blk[:, :, None, :, :]
    inner_out = jnp.einsum('sckmh,scmhp->sckhp', mixing, val_blk, precision=highest)
    closing = cum_log[:, :, -1, :]
    weights_end = jnp.exp(closing[:, :, None, :] - cum_log) * step_blk
    block_states = jnp.einsum('sclh,sclhp,scln->schpn', weights_end, val_blk, in_b, precision=highest)

    def advance(carried, pair):
        factor, added = pair
        return (factor[:, :, None, None] * carried + added, carried)
    final, entering = lax.scan(advance, initial, (jnp.moveaxis(jnp.exp(closing), 1, 0), jnp.moveaxis(block_states, 1, 0)))
    entering = jnp.moveaxis(entering, 0, 1)
    outer_out = jnp.exp(cum_log)[..., None] * jnp.einsum('scln,schpn->sclhp', in_c, entering, precision=highest)
    result = inner_out + outer_out + skips[:, None] * val_blk
    return (result.reshape(batch, length, heads_here, P_SIZE), final)

def silu_slope(values):
    sig = jax.nn.sigmoid(values)
    return sig * (1.0 + values * (1.0 - sig))

def reference(hidden, norm_gain, w_in, conv_w, conv_bias, dt_bias, a_log, d_skip, gate_gain, w_out, cotangent):
    taps = conv_w.astype(jnp.float32)

    def sequence_step(totals, pair):
        hid, cot = pair
        h_float = hid.astype(jnp.float32)
        scale = lax.rsqrt(lax.optimization_barrier(jnp.mean(h_float * h_float, axis=-1, keepdims=True)) + epsilon)
        base = h_float * scale
        normed = (base * norm_gain.astype(jnp.float32)).astype(jnp.bfloat16)
        projected = jnp.dot(normed, w_in, preferred_element_type=jnp.float32).astype(jnp.bfloat16)
        gate_in = projected[:, :DI]
        conv_in = projected[:, DI:DI + XBC]
        dt_raw = projected[:, DI + XBC:]
        padded = jnp.concatenate([jnp.zeros((KW - 1, XBC), jnp.float32), conv_in.astype(jnp.float32)], axis=0)
        pre_act = jnp.broadcast_to(conv_bias.astype(jnp.float32), (SEQ_LEN, XBC))
        for offset in range(KW):
            pre_act = pre_act + taps[:, offset] * padded[offset:offset + SEQ_LEN]
        conv_out = (pre_act * jax.nn.sigmoid(pre_act)).astype(jnp.bfloat16)
        values = conv_out[:, :DI].astype(jnp.float32).reshape(1, SEQ_LEN, H, P_SIZE)
        dt_in = dt_raw.astype(jnp.float32) + dt_bias
        steps = jax.nn.softplus(dt_in)[None]
        rates = -jnp.exp(a_log)
        in_b = conv_out[:, DI:DI + N].astype(jnp.float32)[None]
        in_c = conv_out[:, DI + N:].astype(jnp.float32)[None]
        initial = jnp.zeros((1, H, P_SIZE, N), jnp.float32)
        (scan_out, final), pull = jax.vjp(state_space, values, steps, rates, in_b, in_c, d_skip, initial)
        scanned = scan_out.reshape(SEQ_LEN, DI).astype(jnp.bfloat16)
        scanned_f = scanned.astype(jnp.float32)
        z_float = gate_in.astype(jnp.float32)
        z_sig = jax.nn.sigmoid(z_float)
        gated = scanned_f * z_float * z_sig
        gscale = lax.rsqrt(lax.optimization_barrier(jnp.mean(gated * gated, axis=-1, keepdims=True)) + epsilon)
        gbase = gated * gscale
        gnormed = (gbase * gate_gain.astype(jnp.float32)).astype(jnp.bfloat16)
        branch = jnp.dot(gnormed, w_out, preferred_element_type=jnp.float32)
        output = (h_float + branch).astype(jnp.bfloat16)
        grad_wout = jnp.dot(gnormed.T, cot, preferred_element_type=jnp.float32)
        d_gnormed = jnp.dot(cot, w_out.T, preferred_element_type=jnp.float32)
        grad_gate = lax.optimization_barrier(jnp.sum(d_gnormed * gbase, axis=0))
        e_term = d_gnormed * gate_gain.astype(jnp.float32)
        d_gated = gscale * (e_term - gbase * lax.optimization_barrier(jnp.mean(e_term * gbase, axis=-1, keepdims=True)))
        d_scan = d_gated * z_float * z_sig
        d_gate_in = d_gated * scanned_f * silu_slope(z_float)
        d_values, d_steps, d_rates, d_in_b, d_in_c, d_skips, _ = pull((d_scan.reshape(1, SEQ_LEN, H, P_SIZE), jnp.zeros_like(final)))
        d_dt = d_steps[0] * jax.nn.sigmoid(dt_in)
        grad_dtb = lax.optimization_barrier(jnp.sum(d_dt, axis=0))
        grad_alog = d_rates * rates
        d_conv_out = jnp.concatenate([d_values[0].reshape(SEQ_LEN, DI), d_in_b[0], d_in_c[0]], axis=-1)
        d_pre = d_conv_out * silu_slope(pre_act)
        grad_cbias = lax.optimization_barrier(jnp.sum(d_pre, axis=0))
        grad_taps = jnp.stack([lax.optimization_barrier(jnp.sum(d_pre * padded[offset:offset + SEQ_LEN], axis=0)) for offset in range(KW)], axis=1)
        d_ext = jnp.concatenate([d_pre, jnp.zeros((KW - 1, XBC), jnp.float32)], axis=0)
        d_conv_in = jnp.zeros((SEQ_LEN, XBC), jnp.float32)
        for offset in range(KW):
            d_conv_in = d_conv_in + taps[:, offset] * d_ext[KW - 1 - offset:KW - 1 - offset + SEQ_LEN]
        d_projected = jnp.concatenate([d_gate_in, d_conv_in, d_dt], axis=-1).astype(jnp.bfloat16)
        grad_win = jnp.dot(normed.T, d_projected, preferred_element_type=jnp.float32)
        d_normed = jnp.dot(d_projected, w_in.T, preferred_element_type=jnp.float32)
        grad_norm = lax.optimization_barrier(jnp.sum(d_normed * base, axis=0))
        f_term = d_normed * norm_gain.astype(jnp.float32)
        d_h = scale * (f_term - base * lax.optimization_barrier(jnp.mean(f_term * base, axis=-1, keepdims=True)))
        grad_in = (cot.astype(jnp.float32) + d_h).astype(jnp.bfloat16)
        terms = (grad_norm, grad_win, grad_taps, grad_cbias, grad_dtb, grad_alog, d_skips, grad_gate, grad_wout)
        totals = tuple((left + right for left, right in zip(totals, terms)))
        return (totals, (output, grad_in))
    zeros_init = (jnp.zeros((D,), jnp.float32), jnp.zeros((D, PROJ), jnp.float32), jnp.zeros((XBC, KW), jnp.float32), jnp.zeros((XBC,), jnp.float32), jnp.zeros((H,), jnp.float32), jnp.zeros((H,), jnp.float32), jnp.zeros((H,), jnp.float32), jnp.zeros((DI,), jnp.float32), jnp.zeros((DI, D), jnp.float32))
    totals, (outputs, grad_inputs) = lax.scan(sequence_step, zeros_init, (hidden, cotangent))
    return (outputs, grad_inputs, totals[0], totals[1], totals[2], totals[3], totals[4], totals[5], totals[6], totals[7], totals[8])
```

```python
import functools

import jax
import jax.numpy as jnp
from jax import lax
from jax.experimental import pallas as pl
from jax.experimental.pallas import tpu as pltpu
from jax.sharding import PartitionSpec as P

D = 1536
H = 48
P_SIZE = 64
N = 128
KW = 4
DI = 3072
XBC = 3328
PROJ = 6448
CH = 128
HG = 8
LANES = 128

epsilon = 1e-05
highest = lax.Precision.HIGHEST
LOG2E = 1.4426950408889634
f32 = jnp.float32
bf16 = jnp.bfloat16


def contract(a, b, da, db):
    return lax.dot_general(a, b, (((da,), (db,)), ((), ())), preferred_element_type=f32)


def lane_low(shape):
    return lax.broadcasted_iota(jnp.int32, shape, 1) < P_SIZE


def pair_scale(state, low, high):
    return jnp.concatenate([state[:P_SIZE] * low, state[P_SIZE:] * high], axis=0)


def causal_mask():
    rows = lax.broadcasted_iota(jnp.int32, (CH, CH), 0)
    cols = lax.broadcasted_iota(jnp.int32, (CH, CH), 1)
    return rows >= cols


A_COL, B_COL, DT_COL = 0, HG, 2 * HG


def states_kernel(chunks, last_ref, total_ref, x_ref, b_ref, cols_ref, out_ref):
    group = pl.program_id(0)
    low = lane_low((CH, LANES))
    for pair in range(HG // 2):
        state = jnp.zeros((LANES, N), f32)
        lanes = pl.ds(pair * LANES, LANES)
        h0 = group * HG + 2 * pair
        for c in range(chunks):
            rows = pl.ds(c * CH, CH)
            b0 = cols_ref[rows, B_COL + 2 * pair : B_COL + 2 * pair + 1]
            b1 = cols_ref[rows, B_COL + 2 * pair + 1 : B_COL + 2 * pair + 2]
            weight = jnp.exp2(jnp.where(low, last_ref[c, h0] - b0, last_ref[c, h0 + 1] - b1))
            xw = (x_ref[rows, lanes].astype(f32) * weight).astype(bf16)
            added = contract(xw, b_ref[rows, :], 0, 0)
            state = pair_scale(state, total_ref[c, h0], total_ref[c, h0 + 1]) + added
        out_ref[lanes, :] = state.astype(out_ref.dtype)


def outputs_kernel(
    chunks, last_ref, total_ref, skip_ref, x_ref, b_ref, c_ref, cols_ref, brow_ref, init_ref,
    out_ref, score_ref
):
    group = pl.program_id(0)
    low = lane_low((CH, LANES))

    @pl.when(group == 0)
    def _():
        mask = causal_mask()
        for c in range(chunks):
            rows = pl.ds(c * CH, CH)
            scores = contract(c_ref[rows, :], b_ref[rows, :], 1, 1)
            score_ref[c] = jnp.where(mask, scores, 0.0)

    for pair in range(HG // 2):
        lanes = pl.ds(pair * LANES, LANES)
        state = init_ref[lanes, :].astype(f32)
        h0 = group * HG + 2 * pair
        skip = jnp.where(low, skip_ref[0, h0], skip_ref[0, h0 + 1])
        for c in range(chunks):
            rows = pl.ds(c * CH, CH)
            x = x_ref[rows, lanes]
            zero = jnp.zeros_like(x)
            x_low, x_high = jnp.where(low, x, zero), jnp.where(low, zero, x)
            a0 = cols_ref[rows, A_COL + 2 * pair : A_COL + 2 * pair + 1]
            a1 = cols_ref[rows, A_COL + 2 * pair + 1 : A_COL + 2 * pair + 2]
            mixes = []
            for i, a in ((0, a0), (1, a1)):
                brow = brow_ref[2 * pair + i : 2 * pair + i + 1, rows]
                fade = jnp.exp2(jnp.minimum(a - brow, 126.0))
                mixes.append((score_ref[c] * fade).astype(bf16))
            inner = jnp.dot(
                jnp.concatenate(mixes, axis=1),
                jnp.concatenate([x_low, x_high], axis=0),
                preferred_element_type=f32,
            )
            outer = contract(c_ref[rows, :], state.astype(bf16), 1, 1)
            xf = x.astype(f32)
            y = inner + jnp.exp2(jnp.where(low, a0, a1)) * outer + skip * xf
            out_ref[rows, lanes] = y.astype(out_ref.dtype)
            if c < chunks - 1:
                b0 = cols_ref[rows, B_COL + 2 * pair : B_COL + 2 * pair + 1]
                b1 = cols_ref[rows, B_COL + 2 * pair + 1 : B_COL + 2 * pair + 2]
                weight = jnp.exp2(jnp.where(low, last_ref[c, h0] - b0, last_ref[c, h0 + 1] - b1))
                added = contract((xf * weight).astype(bf16), b_ref[rows, :], 0, 0)
                state = pair_scale(state, total_ref[c, h0], total_ref[c, h0 + 1]) + added


def back_states_kernel(chunks, total_ref, g_ref, c_ref, cols_ref, out_ref):
    group = pl.program_id(0)
    low = lane_low((CH, LANES))
    for pair in range(HG // 2):
        lanes = pl.ds(pair * LANES, LANES)
        h0 = group * HG + 2 * pair
        state = jnp.zeros((LANES, N), f32)
        for c in reversed(range(chunks)):
            rows = pl.ds(c * CH, CH)
            a0 = cols_ref[rows, A_COL + 2 * pair : A_COL + 2 * pair + 1]
            a1 = cols_ref[rows, A_COL + 2 * pair + 1 : A_COL + 2 * pair + 2]
            gi = (g_ref[rows, lanes].astype(f32) * jnp.exp2(jnp.where(low, a0, a1))).astype(bf16)
            added = contract(gi, c_ref[rows, :], 0, 0)
            state = pair_scale(state, total_ref[c, h0], total_ref[c, h0 + 1]) + added
        out_ref[lanes, :] = state.astype(out_ref.dtype)


def grads_kernel(
    chunks, last_ref, total_ref, skip_ref, x_ref, g_ref, b_ref, c_ref, cols_ref, arow_ref,
    dtrow_ref, init_ref, later_ref,
    dx_ref, db_ref, dc_ref, col_ref, q_ref, k_ref, dskip_ref,
    score_ref, dscore_ref, state_ref
):
    group = pl.program_id(0)
    low = lane_low((CH, LANES))

    @pl.when(group == 0)
    def _():
        mask = causal_mask()
        for c in range(chunks):
            rows = pl.ds(c * CH, CH)
            scores = contract(c_ref[rows, :], b_ref[rows, :], 1, 1)
            score_ref[c] = jnp.where(mask, scores, 0.0)
        dscore_ref[...] = jnp.zeros_like(dscore_ref)
        db_ref[...] = jnp.zeros_like(db_ref)
        dc_ref[...] = jnp.zeros_like(dc_ref)

    for pair in range(HG // 2):
        lanes = pl.ds(pair * LANES, LANES)
        h0 = group * HG + 2 * pair
        one = 2 * pair
        skip = jnp.where(low, skip_ref[0, h0], skip_ref[0, h0 + 1])
        state = init_ref[lanes, :].astype(f32)
        for c in range(chunks):
            state_ref[c] = state
            if c < chunks - 1:
                rows = pl.ds(c * CH, CH)
                b0 = cols_ref[rows, B_COL + one : B_COL + one + 1]
                b1 = cols_ref[rows, B_COL + one + 1 : B_COL + one + 2]
                weight = jnp.exp2(jnp.where(low, last_ref[c, h0] - b0, last_ref[c, h0 + 1] - b1))
                xw = (x_ref[rows, lanes].astype(f32) * weight).astype(bf16)
                added = contract(xw, b_ref[rows, :], 0, 0)
                state = pair_scale(state, total_ref[c, h0], total_ref[c, h0 + 1]) + added
        back = later_ref[lanes, :].astype(f32)
        skip_sum = jnp.zeros((1, LANES), f32)
        for c in reversed(range(chunks)):
            rows = pl.ds(c * CH, CH)
            x, g = x_ref[rows, lanes], g_ref[rows, lanes]
            xf, gf = x.astype(f32), g.astype(f32)
            zero = jnp.zeros_like(g)
            halves = (jnp.where(low, g, zero), jnp.where(low, zero, g))
            b_blk, c_blk = b_ref[rows, :], c_ref[rows, :]
            a0 = cols_ref[rows, A_COL + one : A_COL + one + 1]
            a1 = cols_ref[rows, A_COL + one + 1 : A_COL + one + 2]
            d0 = cols_ref[rows, DT_COL + one : DT_COL + one + 1]
            d1 = cols_ref[rows, DT_COL + one + 1 : DT_COL + one + 2]
            since = jnp.where(low, a0, a1)
            step = jnp.where(low, d0, d1)
            from_start = jnp.exp2(since)
            to_end = jnp.exp2(jnp.where(low, last_ref[c, h0], last_ref[c, h0 + 1]) - since)
            mixes, row_sums = [], []
            dscore = dscore_ref[c]
            for i, a in ((0, a0), (1, a1)):
                arow = arow_ref[one + i : one + i + 1, rows]
                dtrow = dtrow_ref[one + i : one + i + 1, rows]
                fade = jnp.exp2(jnp.minimum(a - arow, 0.0))
                mix = score_ref[c] * fade
                gx = contract(halves[i], x, 1, 1)
                both = mix * gx
                q_ref[one + i : one + i + 1, rows] = jnp.sum(both, axis=0, keepdims=True)
                row_sums.append(jnp.sum(both * dtrow, axis=1, keepdims=True))
                dscore = dscore + fade * (gx * dtrow)
                mixes.append(mix.astype(bf16))
            dscore_ref[c] = dscore
            u_inner = contract(jnp.concatenate(mixes, axis=0), jnp.concatenate(halves, axis=0), 0, 0)
            back_h = back.astype(bf16)
            u_later = to_end * contract(b_blk, back_h, 1, 1)
            dx = step * (u_inner + u_later) + skip * gf
            dx_ref[rows, lanes] = dx.astype(dx_ref.dtype)
            z = xf * u_later
            state_c = state_ref[c]
            state_h = state_c.astype(bf16)
            gi = gf * from_start
            yz = gi * contract(c_blk, state_h, 1, 1)
            z_low, yz_low = jnp.where(low, z, 0.0), jnp.where(low, yz, 0.0)
            p0 = jnp.sum(z_low, axis=1, keepdims=True)
            p1 = jnp.sum(z - z_low, axis=1, keepdims=True)
            y0 = jnp.sum(yz_low, axis=1, keepdims=True)
            y1 = jnp.sum(yz - yz_low, axis=1, keepdims=True)
            col_ref[rows, one : one + 1] = row_sums[0] + y0
            col_ref[rows, one + 1 : one + 2] = row_sums[1] + y1
            col_ref[rows, HG + one : HG + one + 1] = p0
            col_ref[rows, HG + one + 1 : HG + one + 2] = p1
            gi_h = gi.astype(bf16)
            dc_ref[rows, :] += jnp.dot(gi_h, state_h, preferred_element_type=f32)
            db_ref[rows, :] += jnp.dot(
                (xf * step * to_end).astype(bf16), back_h, preferred_element_type=f32
            )
            prod = state_c * back
            for i, part in ((0, prod[:P_SIZE]), (1, prod[P_SIZE:])):
                total = jnp.sum(jnp.sum(part, axis=0, keepdims=True), axis=1, keepdims=True)
                k_ref[one + i : one + i + 1, rows] = jnp.broadcast_to(
                    total * total_ref[c, h0 + i], (1, CH)
                )
            skip_sum = skip_sum + jnp.sum(xf * gf, axis=0, keepdims=True)
            back = pair_scale(back, total_ref[c, h0], total_ref[c, h0 + 1]) + contract(
                gi_h, c_blk, 0, 0
            )
        dskip_ref[:, lanes] = skip_sum

    @pl.when(group == pl.num_programs(0) - 1)
    def _():
        mask = causal_mask()
        for c in range(chunks):
            rows = pl.ds(c * CH, CH)
            d = jnp.where(mask, dscore_ref[c], 0.0).astype(bf16)
            dc_ref[rows, :] += jnp.dot(d, b_ref[rows, :], preferred_element_type=f32)
            db_ref[rows, :] += contract(d, c_ref[rows, :], 0, 0)


smem = functools.partial(pl.BlockSpec, memory_space=pltpu.SMEM)


def scan_specs(tokens):
    wide = HG * P_SIZE
    return dict(
        x=pl.BlockSpec((tokens, wide), lambda g: (0, g)),
        bc=pl.BlockSpec((tokens, N), lambda g: (0, 0)),
        cols=pl.BlockSpec((None, tokens, 3 * HG), lambda g: (g, 0, 0)),
        rows=pl.BlockSpec((HG, tokens), lambda g: (g, 0)),
        state=pl.BlockSpec((wide, N), lambda g: (g, 0)),
    )


def cost(flops, nbytes):
    return pl.CostEstimate(flops=int(flops), bytes_accessed=int(nbytes), transcendentals=0)


def local_states(x, b, tab, interpret=False):
    tokens, width = x.shape
    s = scan_specs(tokens)
    return pl.pallas_call(
        functools.partial(states_kernel, tokens // CH),
        grid=(width // (HG * P_SIZE),),
        in_specs=[smem(), smem(), s["x"], s["bc"], s["cols"]],
        out_specs=s["state"],
        out_shape=jax.ShapeDtypeStruct((width, N), f32),
        cost_estimate=cost(2 * tokens * width * N * 4, tokens * width * 2),
        name="local_states",
        interpret=interpret,
    )(tab["last"], tab["total"], x, b, tab["cols"])


def scan_outputs(x, b, c, tab, skip, initial, interpret=False):
    tokens, width = x.shape
    s = scan_specs(tokens)
    return pl.pallas_call(
        functools.partial(outputs_kernel, tokens // CH),
        grid=(width // (HG * P_SIZE),),
        in_specs=[smem(), smem(), smem(), s["x"], s["bc"], s["bc"], s["cols"], s["rows"], s["state"]],
        out_specs=s["x"],
        out_shape=jax.ShapeDtypeStruct((tokens, width), bf16),
        scratch_shapes=[pltpu.VMEM((tokens // CH, CH, CH), f32)],
        cost_estimate=cost(2 * tokens * width * N * 16, tokens * width * 4),
        name="scan_outputs",
        interpret=interpret,
    )(tab["last"], tab["total"], skip, x, b, c, tab["cols"], tab["brow"], initial)


def local_back_states(g, c, tab, interpret=False):
    tokens, width = g.shape
    s = scan_specs(tokens)
    return pl.pallas_call(
        functools.partial(back_states_kernel, tokens // CH),
        grid=(width // (HG * P_SIZE),),
        in_specs=[smem(), s["x"], s["bc"], s["cols"]],
        out_specs=s["state"],
        out_shape=jax.ShapeDtypeStruct((width, N), f32),
        cost_estimate=cost(2 * tokens * width * N * 4, tokens * width * 2),
        name="local_back_states",
        interpret=interpret,
    )(tab["total"], g, c, tab["cols"])


def scan_grads(x, g, b, c, tab, skip, initial, later, interpret=False):
    tokens, width = x.shape
    chunks = tokens // CH
    groups = width // (HG * P_SIZE)
    s = scan_specs(tokens)
    col_out = pl.BlockSpec((None, tokens, 2 * HG), lambda i: (i, 0, 0))
    return pl.pallas_call(
        functools.partial(grads_kernel, chunks),
        grid=(groups,),
        in_specs=[smem(), smem(), smem(), s["x"], s["x"], s["bc"], s["bc"], s["cols"], s["rows"],
                  s["rows"], s["state"], s["state"]],
        out_specs=[s["x"], s["bc"], s["bc"], col_out, s["rows"], s["rows"],
                   pl.BlockSpec((1, HG * P_SIZE), lambda i: (0, i))],
        out_shape=[
            jax.ShapeDtypeStruct((tokens, width), bf16),
            jax.ShapeDtypeStruct((tokens, N), f32),
            jax.ShapeDtypeStruct((tokens, N), f32),
            jax.ShapeDtypeStruct((groups, tokens, 2 * HG), f32),
            jax.ShapeDtypeStruct((groups * HG, tokens), f32),
            jax.ShapeDtypeStruct((groups * HG, tokens), f32),
            jax.ShapeDtypeStruct((1, width), f32),
        ],
        scratch_shapes=[pltpu.VMEM((chunks, CH, CH), f32)] * 2 + [pltpu.VMEM((chunks, LANES, N), f32)],
        cost_estimate=cost(2 * tokens * width * N * 32, tokens * width * 8),
        name="scan_grads",
        interpret=interpret,
    )(tab["last"], tab["total"], skip, x, g, b, c, tab["cols"], tab["arow"], tab["dtrow"], initial,
      later)


def scan_table(steps, rates):
    tokens, heads = steps.shape
    chunks, groups = tokens // CH, heads // HG
    tri = (jnp.arange(CH)[:, None] >= jnp.arange(CH)[None, :]).astype(f32)
    logs = (steps * (rates * LOG2E)).reshape(chunks, CH, heads)
    cum = jnp.einsum("ts,csh->cth", tri, logs, precision=highest)
    last = cum[:, -1, :]
    a = cum.reshape(tokens, heads)
    b = a - jnp.log2(steps)
    stacked = jnp.stack([a, b, steps], axis=1).reshape(tokens, 3, groups, HG)
    cols = jnp.transpose(stacked, (2, 0, 1, 3)).reshape(groups, tokens, 3 * HG)
    turned = jnp.transpose(jnp.concatenate([a, b, steps], axis=1))
    return dict(
        last=last, total=jnp.exp2(last), cols=cols, arow=turned[:heads],
        brow=turned[heads : 2 * heads], dtrow=turned[2 * heads :],
        decay=jnp.exp2(jnp.sum(last, axis=0)),
    )


def scan_step_grads(col, q, k, steps, rates):
    groups, tokens, _ = col.shape
    heads = groups * HG
    chunks = tokens // CH
    fix = jnp.transpose(col.reshape(groups, tokens, 2, HG), (1, 2, 0, 3)).reshape(tokens, 2, heads)
    ahead, direct = fix[:, 0], fix[:, 1]
    qt, kt = jnp.transpose(q), jnp.transpose(k)
    tri = (jnp.arange(CH)[:, None] <= jnp.arange(CH)[None, :]).astype(f32)
    below = (jnp.arange(CH)[:, None] > jnp.arange(CH)[None, :]).astype(f32)

    def chunked(v):
        return v.reshape(chunks, CH, heads)

    d_log = jnp.einsum("ts,csh->cth", tri, chunked(ahead - steps * qt), precision=highest)
    d_log = d_log + jnp.einsum("ts,csh->cth", below, chunked(steps * direct), precision=highest)
    d_log = d_log.reshape(tokens, heads) + kt
    return qt + direct + rates * d_log, jnp.sum(steps * d_log, axis=0)


def carry_states(local, decay, reverse):
    ns, nc = lax.axis_size("sp"), lax.axis_size("cp")
    rows = local.shape[0] // ns
    heads = decay.shape[0] // ns
    decays = lax.all_gather(decay, "sp")
    mine = lax.dynamic_slice_in_dim(decays, lax.axis_index("sp") * heads, heads, axis=1)
    wide = jnp.repeat(mine, P_SIZE, axis=1)[:, :, None]
    got = lax.all_to_all(local.astype(bf16).reshape(ns, rows, N), "sp", 0, 0, tiled=True)
    got = got.astype(f32)
    order = list(range(ns))[::-1] if reverse else list(range(ns))
    run = jnp.zeros((rows, N), f32)
    grown = jnp.ones((rows, 1), f32)
    entering, growth = [None] * ns, [None] * ns
    for i in order:
        entering[i], growth[i] = run, grown
        run = wide[i] * run + got[i]
        grown = grown * wide[i]
    outside = jnp.zeros((rows, N), f32)
    shift = [(i, i - 1) for i in range(1, nc)] if reverse else [(i, i + 1) for i in range(nc - 1)]
    for _ in range(nc - 1):
        outside = lax.ppermute((run + grown * outside).astype(bf16), "cp", shift).astype(f32)
    out = jnp.stack([entering[i] + growth[i] * outside for i in range(ns)]).astype(bf16)
    back = lax.all_to_all(out, "sp", 0, 0, tiled=True)
    return back.reshape(local.shape)


MESH = pl.DeviceIdType.MESH
GATHER_CHUNKS = 6
SUM_CHUNKS = 12


class Spot:
    def __init__(self):
        self.me = lax.axis_index("dp")
        self.core = lax.axis_index("cp")
        self.z = lax.axis_index("sp")
        self.x = self.me + 1 - 2 * (self.me % 2)
        self.y = (self.me + 2) % 4
        self.far = 3 - self.me
        self.to_x = {"dp": self.x}
        self.to_y = {"dp": self.y}
        self.to_core = {"cp": 1 - self.core}
        self.to_up = {"sp": self.z + 1}
        self.to_down = {"sp": self.z - 1}


def remote(src, dst, send, recv, to):
    return pltpu.make_async_remote_copy(
        src_ref=src, dst_ref=dst, send_sem=send, recv_sem=recv, device_id=to, device_id_type=MESH
    )


def gather_kernel(windows, *refs):
    n = len(windows)
    nc = GATHER_CHUNKS
    src, dst = refs[:n], refs[n : 2 * n]
    stage = refs[2 * n : 3 * n]
    xs, xr, ys, yr, fs, fr, cs, cr, local = refs[3 * n :]
    s = Spot()
    barrier = pltpu.get_barrier_semaphore()
    for to in (s.to_x, s.to_y, s.to_core):
        pl.semaphore_signal(barrier, inc=1, device_id=to, device_id_type=MESH)
    pl.semaphore_wait(barrier, 3)

    def at(i, block, core, j):
        rows, _, _ = windows[i]
        size = rows // 2 // nc
        return dst[i].at[pl.ds(pl.multiple_of(block * rows + core * (rows // 2) + j * size, 16), size), :]

    def own(i, j):
        rows, first, cols = windows[i]
        size = rows // 2 // nc
        return src[i].at[
            pl.ds(pl.multiple_of(s.core * (rows // 2) + j * size, 16), size), pl.ds(first, cols)
        ]

    def by_x(i, j):
        return remote(own(i, j), at(i, s.me, s.core, j), xs.at[i, j], xr.at[i, j], s.to_x)

    def by_y(i, j):
        return remote(own(i, j), at(i, s.me, s.core, j), ys.at[i, j], yr.at[i, j], s.to_y)

    def onward(i, j):
        if j % 2 == 0:
            here = at(i, s.x, s.core, j)
            return remote(here, here, fs.at[i, j], fr.at[i, j], s.to_y)
        here = at(i, s.y, s.core, j)
        return remote(here, here, fs.at[i, j], fr.at[i, j], s.to_x)

    def cross(i, kind, j):
        block = (s.x, s.y, s.far)[kind]
        here = at(i, block, s.core, j)
        return remote(here, here, cs.at[i, kind, j], cr.at[i, kind, j], s.to_core)

    loads = []
    for i in range(n):
        rows, first, cols = windows[i]
        loads.append(
            pltpu.make_async_copy(src[i].at[:, pl.ds(first, cols)], stage[i], local.at[i, 0])
        )
        loads[-1].start()
    steps = [(i, j) for i in range(n) for j in range(nc)]
    lag = 2
    for t in range(len(steps) + 2 * lag):
        if t < len(steps):
            i, j = steps[t]
            by_x(i, j).start()
            by_y(i, nc - 1 - j).start()
        if 0 <= t - lag < len(steps):
            i, j = steps[t - lag]
            other = nc - 1 - j
            by_x(i, j).wait_recv()
            if j % 2 == 0:
                onward(i, j).start()
            by_y(i, other).wait_recv()
            if other % 2 == 1:
                onward(i, other).start()
            cross(i, 0, j).start()
            cross(i, 1, other).start()
        if 0 <= t - 2 * lag < len(steps):
            i, j = steps[t - 2 * lag]
            if j % 2 == 0:
                for jj in (j, nc - 1 - j):
                    onward(i, jj).wait_recv()
                    cross(i, 2, jj).start()
    stores = []
    for i in range(n):
        rows = windows[i][0]
        loads[i].wait()
        stores.append(
            pltpu.make_async_copy(
                stage[i], dst[i].at[pl.ds(pl.multiple_of(s.me * rows, 16), rows), :], local.at[i, 1]
            )
        )
        stores[-1].start()
    for i, j in steps:
        for kind in range(3):
            cross(i, kind, j).wait()
        by_x(i, j).wait_send()
        by_y(i, j).wait_send()
        onward(i, j).wait_send()
    for store in stores:
        store.wait()


def gather_weights(arrays, windows):
    n, nc = len(arrays), GATHER_CHUNKS
    any_spec = pl.BlockSpec(memory_space=pl.ANY)
    sems = [pltpu.SemaphoreType.DMA((n, nc))] * 6 + [pltpu.SemaphoreType.DMA((n, 3, nc))] * 2
    return pl.pallas_call(
        functools.partial(gather_kernel, windows),
        in_specs=[any_spec] * n,
        out_specs=[any_spec] * n,
        out_shape=[jax.ShapeDtypeStruct((4 * r, c), bf16) for r, _, c in windows],
        scratch_shapes=[pltpu.VMEM((r, c), bf16) for r, _, c in windows]
        + sems + [pltpu.SemaphoreType.DMA((n, 2))],
        compiler_params=pltpu.CompilerParams(collective_id=1, has_side_effects=True),
        name="gather_weights",
    )(*arrays)


SUM_BUFFERS = 9
SUM_SEMS = 23


def sum_kernel(shapes, *refs):
    n, nc = len(shapes), SUM_CHUNKS
    src, dst = refs[:n], refs[n : 2 * n]
    rest = refs[2 * n :]
    per = SUM_BUFFERS + SUM_SEMS
    held = [rest[i * per : (i + 1) * per] for i in range(n)]
    s = Spot()
    z = s.z
    ns = 4
    barrier = pltpu.get_barrier_semaphore()
    for to in (s.to_x, s.to_y, s.to_core):
        pl.semaphore_signal(barrier, inc=1, device_id=to, device_id_type=MESH)

    @pl.when(z > 0)
    def _():
        pl.semaphore_signal(barrier, inc=1, device_id=s.to_down, device_id_type=MESH)

    @pl.when(z < ns - 1)
    def _():
        pl.semaphore_signal(barrier, inc=1, device_id=s.to_up, device_id_type=MESH)

    pl.semaphore_wait(barrier, 3 + (z > 0).astype(jnp.int32) + (z < ns - 1).astype(jnp.int32))

    def moves(i):
        rows, cols, left = shapes[i]
        size = rows // 2 // nc
        (mine, theirs, xin, yin, x2, y2, up, down, fin,
         ls, ps, pr, xs0, xr0, xs1, xr1, ys0, yr0, ys1, yr1, x2s, x2r, y2s, y2r,
         ups, upr, dns, dnr, fus, fds, fr, misc) = held[i]
        lo, hi = pl.ds(0, left), pl.ds(left, cols - left)

        def rows_of(core, j):
            return pl.ds(pl.multiple_of(core * (rows // 2) + j * size, 16), size)

        def m(name, j):
            return {
                "load": lambda: pltpu.make_async_copy(
                    src[i].at[:, rows_of(s.core, j), :], mine.at[j], ls.at[j]),
                "pair": lambda: remote(
                    src[i].at[:, rows_of(1 - s.core, j), :], theirs.at[j], ps.at[j], pr.at[j], s.to_core),
                "x0": lambda: remote(mine.at[j, s.x, :, lo], xin.at[j, 0], xs0.at[j], xr0.at[j], s.to_x),
                "x1": lambda: remote(mine.at[j, s.far, :, lo], xin.at[j, 1], xs1.at[j], xr1.at[j], s.to_x),
                "y0": lambda: remote(mine.at[j, s.y, :, hi], yin.at[j, 0], ys0.at[j], yr0.at[j], s.to_y),
                "y1": lambda: remote(mine.at[j, s.far, :, hi], yin.at[j, 1], ys1.at[j], yr1.at[j], s.to_y),
                "y2": lambda: remote(mine.at[j, s.y, :, lo], y2.at[j], y2s.at[j], y2r.at[j], s.to_y),
                "x2": lambda: remote(mine.at[j, s.x, :, hi], x2.at[j], x2s.at[j], x2r.at[j], s.to_x),
                "up": lambda: remote(mine.at[j, s.me], up.at[j], ups.at[j], upr.at[j], s.to_up),
                "down": lambda: remote(mine.at[j, s.me], down.at[j], dns.at[j], dnr.at[j], s.to_down),
                "fup": lambda: remote(fin.at[j], fin.at[j], fus.at[j], fr.at[j], s.to_up),
                "fdown": lambda: remote(fin.at[j], fin.at[j], fds.at[j], fr.at[j], s.to_down),
                "out": lambda: pltpu.make_async_copy(
                    fin.at[j], dst[i].at[rows_of(s.core, j), :], misc.at[0, j]),
                "share": lambda: remote(
                    fin.at[j], dst[i].at[rows_of(s.core, j), :], misc.at[1, j], misc.at[2, j], s.to_core),
            }[name]()

        return m, held[i][:SUM_BUFFERS], lo, hi

    def add(a, b):
        return (a.astype(f32) + b.astype(f32)).astype(bf16)

    def step(i, t):
        m, (mine, theirs, xin, yin, x2, y2, up, down, fin), lo, hi = moves(i)

        def stage(j, more=True):
            ok = (j >= 0) & (j < nc)
            return pl.when(ok if more is True else ok & more)

        @stage(t)
        def _():
            m("load", t).start()
            m("pair", t).start()

        j1 = t - 2

        @stage(j1)
        def _():
            m("load", j1).wait()
            m("pair", j1).wait_recv()
            for b in range(4):
                mine[j1, b] = add(mine[j1, b], theirs[j1, b])
            for name in ("x1", "y1", "x0", "y0"):
                m(name, j1).start()

        j2 = t - 4

        @stage(j2)
        def _():
            for name in ("x1", "y1", "x0", "y0"):
                m(name, j2).wait_recv()
            mine[j2, s.y, :, lo] = add(mine[j2, s.y, :, lo], xin[j2, 1])
            m("y2", j2).start()
            mine[j2, s.x, :, hi] = add(mine[j2, s.x, :, hi], yin[j2, 1])
            m("x2", j2).start()
            mine[j2, s.me, :, lo] = add(mine[j2, s.me, :, lo], xin[j2, 0])
            mine[j2, s.me, :, hi] = add(mine[j2, s.me, :, hi], yin[j2, 0])

        j3 = t - 6

        @stage(j3)
        def _():
            m("y2", j3).wait_recv()
            m("x2", j3).wait_recv()
            mine[j3, s.me, :, lo] = add(mine[j3, s.me, :, lo], y2[j3])
            mine[j3, s.me, :, hi] = add(mine[j3, s.me, :, hi], x2[j3])

        ju = t - 6 - z
        owner_u = (ju + 2 * i + 4 * ns) % ns

        @stage(ju, z <= owner_u)
        def _():
            @pl.when(z > 0)
            def _():
                m("up", ju).wait_recv()
                mine[ju, s.me] = add(mine[ju, s.me], up[ju])

            @pl.when(z < owner_u)
            def _():
                m("up", ju).start()

        jd = t - 6 - (ns - 1) + z
        owner_d = (jd + 2 * i + 4 * ns) % ns

        @stage(jd, z >= owner_d)
        def _():
            @pl.when(z < ns - 1)
            def _():
                m("down", jd).wait_recv()
                mine[jd, s.me] = add(mine[jd, s.me], down[jd])

            @pl.when(z > owner_d)
            def _():
                m("down", jd).start()

        jo = t - 6 - (ns - 1)
        owner_o = (jo + 2 * i + 4 * ns) % ns

        @stage(jo, z == owner_o)
        def _():
            fin[jo] = mine[jo, s.me]

            @pl.when(z < ns - 1)
            def _():
                m("fup", jo).start()

            @pl.when(z > 0)
            def _():
                m("fdown", jo).start()

        jfu = t - 9 - z
        owner_fu = (jfu + 2 * i + 4 * ns) % ns

        @stage(jfu, owner_fu < z)
        def _():
            m("fup", jfu).wait_recv()

            @pl.when(z < ns - 1)
            def _():
                m("fup", jfu).start()

        jfd = t - 9 - (ns - 1) + z
        owner_fd = (jfd + 2 * i + 4 * ns) % ns

        @stage(jfd, owner_fd > z)
        def _():
            m("fdown", jfd).wait_recv()

            @pl.when(z > 0)
            def _():
                m("fdown", jfd).start()

        je = t - 13

        @stage(je)
        def _():
            m("out", je).start()
            m("share", je).start()

    def run(t, carry):
        for i in range(n):
            step(i, t - i * nc)
        return carry

    lax.fori_loop(0, n * nc + 13, run, 0)

    def finish(j, carry):
        for i in range(n):
            m = moves(i)[0]
            owner = (j + 2 * i) % ns
            m("out", j).wait()
            m("share", j).wait()
            for name in ("pair", "x0", "x1", "y0", "y1", "x2", "y2"):
                m(name, j).wait_send()
            for name, cond in (
                ("up", z < owner), ("down", z > owner),
                ("fup", (z >= owner) & (z < ns - 1)), ("fdown", (z <= owner) & (z > 0)),
            ):
                @pl.when(cond)
                def _(name=name):
                    m(name, j).wait_send()
        return carry

    lax.fori_loop(0, nc, finish, 0)


def sum_grads(grads, lefts):
    nc = SUM_CHUNKS
    any_spec = pl.BlockSpec(memory_space=pl.ANY)
    shapes = [(g.shape[0] // 4, g.shape[1], left) for g, left in zip(grads, lefts)]
    scratch = []
    for rows, cols, left in shapes:
        size = rows // 2 // nc
        right = cols - left
        scratch += [
            pltpu.VMEM((nc, 4, size, cols), bf16), pltpu.VMEM((nc, 4, size, cols), bf16),
            pltpu.VMEM((nc, 2, size, left), bf16), pltpu.VMEM((nc, 2, size, right), bf16),
            pltpu.VMEM((nc, size, right), bf16), pltpu.VMEM((nc, size, left), bf16),
            pltpu.VMEM((nc, size, cols), bf16), pltpu.VMEM((nc, size, cols), bf16),
            pltpu.VMEM((nc, size, cols), bf16),
        ]
        scratch += [pltpu.SemaphoreType.DMA((nc,))] * (SUM_SEMS - 1)
        scratch += [pltpu.SemaphoreType.DMA((3, nc))]
    return pl.pallas_call(
        functools.partial(sum_kernel, shapes),
        in_specs=[any_spec] * len(grads),
        out_specs=[any_spec] * len(grads),
        out_shape=[jax.ShapeDtypeStruct((r, c), bf16) for r, c, _ in shapes],
        scratch_shapes=scratch,
        compiler_params=pltpu.CompilerParams(
            collective_id=2, has_side_effects=True, vmem_limit_bytes=66 * 1024 * 1024
        ),
        name="sum_grads",
    )(*[g.reshape(4, g.shape[0] // 4, g.shape[1]) for g in grads])


def shifted(array, axis, by):
    length = lax.axis_size(axis) if isinstance(axis, str) else lax.axis_size(axis[0]) * lax.axis_size(axis[1])
    pairs = [(i, i + by) for i in range(length) if 0 <= i + by < length]
    return lax.ppermute(array, axis, pairs)


def small_ring():
    return (lax.axis_size("dp"), lax.axis_size("cp"), lax.axis_size("sp")) == (4, 2, 4)


def gather_all(arrays, windows):
    if small_ring():
        return gather_weights(arrays, windows)
    return [
        lax.all_gather(a[:, first : first + cols], "dp", axis=0, tiled=True)
        for a, (_, first, cols) in zip(arrays, windows)
    ]


def sum_all(grads, lefts):
    if small_ring():
        return sum_grads(grads, lefts)
    return [
        lax.psum(lax.psum_scatter(g, "dp", scatter_dimension=0, tiled=True), ("cp", "sp"))
        for g in grads
    ]


def silu_slope(values):
    sig = jax.nn.sigmoid(values)
    return sig * (1.0 + values * (1.0 - sig))


def as_columns(v, groups, rows):
    v = v.reshape(groups, -1)
    count = -(-v.shape[1] // rows)
    v = jnp.pad(v, ((0, 0), (0, count * rows - v.shape[1])))
    return jnp.transpose(v.reshape(groups, count, rows), (0, 2, 1))


def from_columns(block, length):
    flat = jnp.transpose(block, (0, 2, 1)).reshape(block.shape[0], -1)
    return flat[:, :length]


def body(
    hidden, norm_gain, w_in, conv_w, conv_bias, dt_bias, a_log, d_skip, gate_gain, w_out, cotangent
):
    tokens = hidden.shape[0] * hidden.shape[1]
    groups = lax.axis_size("dp")
    rows_in = w_in.shape[0]
    lens = [norm_gain.shape[0], gate_gain.shape[0], conv_bias.shape[0], conv_w.size]
    counts = [-(-length // rows_in) for length in lens]
    cuts = [H + sum(counts[:i]) for i in range(len(lens) + 1)]
    wide = XBC + LANES

    def packed(vectors):
        cols = [as_columns(v, 1, rows_in)[0] for v in vectors]
        return jnp.concatenate(cols, axis=1)

    extra = packed([norm_gain, gate_gain, conv_bias, jnp.transpose(conv_w).reshape(-1)])
    pad = jnp.zeros((rows_in, LANES - H - extra.shape[1]), bf16)
    shard = jnp.concatenate([w_in[:, DI:], extra, pad], axis=1)
    w_conv, w_gate, full_out = gather_all(
        [shard, w_in, w_out],
        [(rows_in, 0, wide), (rows_in, 0, DI), (w_out.shape[0], 0, w_out.shape[1])],
    )
    small = w_conv[:, XBC:].reshape(groups, rows_in, LANES)
    pieces = [
        from_columns(small[:, :, cuts[i] : cuts[i + 1]], lens[i]) for i in range(len(lens))
    ]
    full_norm = pieces[0].reshape(-1).astype(f32)
    full_gate = pieces[1].reshape(-1).astype(f32)
    full_bias = pieces[2].reshape(-1).astype(f32)
    taps = jnp.transpose(pieces[3].reshape(groups, KW, -1), (1, 0, 2)).reshape(KW, XBC).astype(f32)

    hid = hidden.reshape(tokens, D)
    cot = cotangent.reshape(tokens, D)
    h_float = hid.astype(f32)
    scale = lax.rsqrt(jnp.mean(h_float * h_float, axis=-1, keepdims=True) + epsilon)
    base = h_float * scale
    normed = (base * full_norm).astype(bf16)
    projected = jnp.dot(normed, w_conv, preferred_element_type=f32).astype(bf16)
    conv_in, dt_raw = projected[:, :XBC], projected[:, XBC : XBC + H]

    prior = shifted(conv_in[tokens - (KW - 1) :], ("cp", "sp"), 1)
    padded = jnp.concatenate([prior, conv_in], axis=0).astype(f32)
    pre_act = jnp.broadcast_to(full_bias, (tokens, XBC))
    for k in range(KW):
        pre_act = pre_act + taps[k] * padded[k : k + tokens]
    conv_out = (pre_act * jax.nn.sigmoid(pre_act)).astype(bf16)
    x, in_b, in_c = conv_out[:, :DI], conv_out[:, DI : DI + N], conv_out[:, DI + N :]

    dt_in = dt_raw.astype(f32) + dt_bias
    steps = jax.nn.softplus(dt_in)
    rates = -jnp.exp(a_log)
    tab = scan_table(steps, rates)
    skip = d_skip[None]
    ends = local_states(x, in_b, tab)
    initial = carry_states(ends, tab["decay"], False)
    scanned = scan_outputs(x, in_b, in_c, tab, skip, initial)

    gate_in = jnp.dot(normed, w_gate, preferred_element_type=f32).astype(bf16)
    scanned_f = scanned.astype(f32)
    z_float = gate_in.astype(f32)
    z_sig = jax.nn.sigmoid(z_float)
    gated = scanned_f * z_float * z_sig
    gscale = lax.rsqrt(jnp.mean(gated * gated, axis=-1, keepdims=True) + epsilon)
    gbase = gated * gscale
    gnormed = (gbase * full_gate).astype(bf16)
    branch = jnp.dot(gnormed, full_out, preferred_element_type=f32)
    out_hidden = (h_float + branch).astype(bf16)
    d_gnormed = contract(cot, full_out, 1, 1)
    grad_gate = jnp.sum(d_gnormed * gbase, axis=0)
    e_term = d_gnormed * full_gate
    d_gated = gscale * (e_term - gbase * jnp.mean(e_term * gbase, axis=-1, keepdims=True))
    d_scan = (d_gated * z_float * z_sig).astype(bf16)
    d_gate_in = (d_gated * scanned_f * silu_slope(z_float)).astype(bf16)

    starts = local_back_states(d_scan, in_c, tab)
    later = carry_states(starts, tab["decay"], True)
    grad_wout = contract(gnormed, cot, 0, 0).astype(bf16)
    grad_wgate = contract(normed, d_gate_in, 0, 0).astype(bf16)

    dx, d_b, d_c, col, q, k, dskip = scan_grads(
        x, d_scan, in_b, in_c, tab, skip, initial, later
    )
    d_steps, d_rates = scan_step_grads(col, q, k, steps, rates)
    d_dt = d_steps * jax.nn.sigmoid(dt_in)
    d_conv_out = jnp.concatenate([dx.astype(f32), d_b, d_c], axis=-1)
    d_pre = d_conv_out * silu_slope(pre_act)
    grad_cbias = jnp.sum(d_pre, axis=0)
    grad_taps = jnp.stack([jnp.sum(d_pre * padded[i : i + tokens], axis=0) for i in range(KW)])
    after = shifted(d_pre[: KW - 1].astype(bf16), ("cp", "sp"), -1).astype(f32)
    d_ext = jnp.concatenate([d_pre, after], axis=0)
    d_conv_in = jnp.zeros((tokens, XBC), f32)
    for i in range(KW):
        d_conv_in = d_conv_in + taps[i] * d_ext[KW - 1 - i : KW - 1 - i + tokens]
    d_proj = jnp.concatenate(
        [d_conv_in.astype(bf16), d_dt.astype(bf16), jnp.zeros((tokens, LANES - H), bf16)], axis=1
    )
    grad_wconv = contract(normed, d_proj, 0, 0).astype(bf16)
    d_normed = contract(d_gate_in, w_gate, 1, 1) + contract(d_proj, w_conv, 1, 1)
    grad_norm = jnp.sum(d_normed * base, axis=0)
    f_term = d_normed * full_norm
    d_h = scale * (f_term - base * jnp.mean(f_term * base, axis=-1, keepdims=True))
    grad_hidden = (cot.astype(f32) + d_h).astype(bf16)

    turned = jnp.transpose(grad_taps.reshape(KW, groups, -1), (1, 0, 2))
    extra = jnp.concatenate(
        [as_columns(v, groups, rows_in) for v in (grad_norm, grad_gate, grad_cbias, turned)], axis=2
    ).astype(bf16)
    grad_wconv = lax.dynamic_update_slice(
        grad_wconv, extra.reshape(groups * rows_in, -1), (0, XBC + H)
    )
    own_wout, own_wgate, own_wconv = sum_all(
        [grad_wout, grad_wgate, grad_wconv], [D // 2, DI // 2, 14 * LANES]
    )
    own = [
        from_columns(own_wconv[None, :, XBC + cuts[i] : XBC + cuts[i + 1]], lens[i])[0].astype(f32)
        for i in range(len(lens))
    ]
    own_win = jnp.concatenate([own_wgate, own_wconv[:, : XBC + H]], axis=1).astype(f32)
    heads = jnp.stack(
        [jnp.sum(d_dt, axis=0), d_rates * rates, jnp.sum(dskip.reshape(H, P_SIZE), axis=1)]
    )
    heads = lax.psum(heads, ("dp", "cp", "sp"))
    return (
        out_hidden.reshape(hidden.shape), grad_hidden.reshape(hidden.shape), own[0],
        own_win, jnp.transpose(own[3].reshape(KW, -1)), own[2], heads[0], heads[1], heads[2],
        own[1], own_wout.astype(f32),
    )


def solution(mesh):
    rows, own = P("dp", ("cp", "sp"), None), P("dp")
    block = P("dp", None)
    in_specs = (rows, own, block, block, own, P(), P(), P(), own, block, rows)
    out_specs = (rows, rows, own, block, block, own, P(), P(), P(), own, block)
    return jax.shard_map(body, mesh=mesh, in_specs=in_specs, out_specs=out_specs, check_vma=False)
```
